32 devices in a mesh: dp: 2 (over y), expert: 16 (over z, x, core).
Axes of the slice: x: 2, y: 2, z: 4, core: 2. Of those that a mesh axis runs over, the one named last changes fastest.
Arguments:
- tokens: bfloat16 [4096, 2048], P(('dp', 'expert')), may hold values from -6 to 6
- out_grad: bfloat16 [4096, 2048], P(('dp', 'expert')), may hold values from -6 to 6
- expert_ids: int32 [4096, 2], P(('dp', 'expert')), may hold values from 0 to 15, all different within a row; in each aligned block of 128 rows (0 to 127, 128 to 255, ...) at most 32 rows name the same one
- gate_probs: float32 [4096, 2], P(('dp', 'expert')), may hold values from 0.1 to 1
- held_expert: int32 [16], replicated, may hold values from 0 to 15, each once
- swap_pairs: int32 [4], replicated, may hold values from 0 to 7, as said below
- w_in: bfloat16 [16, 2048, 1536], P('expert', 'dp'), may hold values from -0.125 to 0.125
- w_down: bfloat16 [16, 2048, 768], P('expert', 'dp'), may hold values from -0.21875 to 0.21875
- m_in: bfloat16 [16, 2048, 1536], P('expert', 'dp'), may hold values from -12 to 12
- m_down: bfloat16 [16, 2048, 768], P('expert', 'dp'), may hold values from -12 to 12
- v_in: bfloat16 [16, 2048, 1536], P('expert', 'dp'), may hold values from 4 to 400
- v_down: bfloat16 [16, 2048, 768], P('expert', 'dp'), may hold values from 4 to 400
Outputs:
- token_grad: bfloat16 [4096, 2048], P(('dp', 'expert'))
- prob_grad: float32 [4096, 2], P(('dp', 'expert'))
- new_w_in: bfloat16 [16, 2048, 1536], P('expert', 'dp')
- new_w_down: bfloat16 [16, 2048, 768], P('expert', 'dp')
- new_m_in: bfloat16 [16, 2048, 1536], P('expert', 'dp')
- new_m_down: bfloat16 [16, 2048, 768], P('expert', 'dp')
- new_v_in: bfloat16 [16, 2048, 1536], P('expert', 'dp')
- new_v_down: bfloat16 [16, 2048, 768], P('expert', 'dp')
The draws below stay inside these ranges and needn't reach their ends.
Inputs may be any that keep to these rules, and one draw needn't show every extreme that they name: `expert_ids`: each row names 2 different experts; among the 128 rows of one device no expert is named by more than 32 rows, and some expert reaches 32. `held_expert`: A permutation of the experts. `swap_pairs`: 4 different values; value p stands for the slots p and p + 8.
All inputs are finite; a program needn't handle non-finite values.
Results may differ from the reference program's by a relative error of at most 0.02.
Values may be sent and summed in bfloat16 or wider, within the bound.
No kernel may reach another device: no remote copies, remote signals or barrier semaphores. Data moves between devices by JAX's collectives and lax.ppermute only.
A program may use at most 128 MiB of HBM per device.

```python
import math
import jax
import jax.numpy as jnp
import numpy as np
from jax import lax

D = 2048
H = 768
TOP = 2
PAIRS = 4
TOK_DEV = 128
EXPERTS = 16
CAP = 32
TOKENS = 4096
N_DP = 2


def draw_swap_pairs(key, part):
    half_count = EXPERTS // 2
    middle = jax.random.permutation(jax.random.fold_in(key, 7), half_count - 2) + 1
    chosen = jnp.concatenate([jnp.array([0, half_count - 1], jnp.int32), middle[:PAIRS - 2].astype(jnp.int32)])
    return jax.random.permutation(jax.random.fold_in(key, 11), chosen).astype(jnp.int32)


def level_of(rng, extent, shards, smallest, top_value):
    def one(axis_at, blocks):
        heights = jax.random.uniform(jax.random.fold_in(jax.random.fold_in(rng, 6), axis_at), (blocks,), jnp.float32, smallest / len(shards), top_value / len(shards))
        return jnp.repeat(jnp.exp(heights), extent[axis_at] // blocks).reshape((-1,) + (1,) * (len(extent) - axis_at - 1))

    factor_of = one(*shards[0])
    for cut in shards[1:]:
        factor_of = factor_of * one(*cut)
    return factor_of


def routed_block(own_key, own, number, rows, amount, top, bound, lean):
    sequence = jax.random.permutation(own_key, amount)
    crowded, usual = shares(amount, rows * top, bound, lean, True), shares(amount, rows * top, bound, lean, False)
    places = jnp.arange(amount)

    def named(lengths, rotation):
        used = int((lengths > 0).sum())
        fixed = max(1, used // 4)
        passed = fixed + (places - fixed + rotation * (used - fixed)) % max(1, amount - fixed)
        return jnp.zeros((amount,), jnp.int32).at[sequence[jnp.where(places < fixed, places, passed)]].set(jnp.asarray(lengths, jnp.int32))

    lengths = jnp.where(number % 4 == 0, named(crowded, number // 4), named(usual, number - number // 4 - 1))
    mixed = jax.random.permutation(jax.random.fold_in(own, 3), amount)
    donor, sink = mixed[0:amount // 2 * 2:2], mixed[1:amount // 2 * 2:2]
    margin = jnp.minimum(lengths[donor] - 1, bound - lengths[sink]) // 2
    margin = jnp.where((donor == sequence[0]) | (sink == sequence[0]) | (lengths[sink] == 0), 0, jnp.maximum(margin, 0))
    passed = jax.random.randint(jax.random.fold_in(own, 4), (amount // 2,), 0, 1 << 20) % (margin + 1)
    lengths = lengths.at[donor].add(-passed).at[sink].add(passed)
    items = jnp.searchsorted(jnp.cumsum(lengths), jnp.arange(rows * top), side="right").astype(jnp.int32)
    grid = items.reshape(top, rows).T
    grid = grid[jax.random.permutation(jax.random.fold_in(own, 1), rows)]
    rotation = jax.random.randint(jax.random.fold_in(own, 2), (rows, 1), 0, top)
    return jnp.take_along_axis(grid, (jnp.arange(top)[None, :] + rotation) % top, axis=1)


def shares(number_of, total, most, slope, full):
    loads = [(1 << 20) // math.isqrt(rank ** slope) + 1 for rank in range(1, number_of + 1)]
    largest = most if full else min(most, max(-(-total // number_of), total * loads[0] // sum(loads)))
    least = 1 if total - largest >= number_of - 1 else 0
    given, rest = [largest] + [least] * (number_of - 1), total - largest - least * (number_of - 1)
    while rest > 0:
        movable = [i for i in range(1, number_of) if given[i] < largest] or [i for i in range(1, number_of) if given[i] < most]
        whole, remaining = sum([loads[i] for i in movable]), rest
        for i in movable:
            addition = min(most - given[i], max(1, remaining * loads[i] // whole), rest)
            given[i] = given[i] + addition
            rest = rest - addition
    return np.array(given)


def centred(rng, dims, deviation, most, pieces=(), held_as=jnp.bfloat16):
    values = jax.random.normal(rng, dims, jnp.float32) * deviation
    if len(pieces) > 0:
        values = level_of(rng, dims, pieces, -0.22, 0.18) * values
    return jnp.clip(values, min=-most, max=most).astype(held_as)


def setup_inputs(seed: int = 0) -> dict:
    seeds = jax.random.split(jax.random.key(seed), 13)
    tokens = centred(seeds[0], (TOKENS, D), 1.0, 6.0, ((0, 32),))
    out_grad = centred(seeds[1], (TOKENS, D), 1.0, 6.0, ((0, 32),))
    expert_ids_keys = jax.random.split(jax.random.fold_in(seeds[2], 1), TOKENS // TOK_DEV)
    expert_ids_turns = jax.random.permutation(jax.random.fold_in(seeds[2], 3), TOKENS // TOK_DEV)
    expert_ids = jax.vmap(lambda own, number: routed_block(jax.random.fold_in(seeds[2], 2), own, number, TOK_DEV, EXPERTS, TOP, CAP, 2))(expert_ids_keys, expert_ids_turns).reshape((TOKENS, TOP))
    gate_probs = jnp.clip(0.1 + 0.9 * jax.random.uniform(seeds[3], (TOKENS, TOP), jnp.float32) ** level_of(seeds[3], (TOKENS, TOP), ((0, 32),), -0.2, 0.2), 0.1, 1.0)
    held_expert = jax.random.permutation(seeds[4], EXPERTS).astype(jnp.int32)
    swap_pairs = draw_swap_pairs(jax.random.fold_in(seeds[12], 71), 0)
    w_in = centred(seeds[6], (EXPERTS, D, 2 * H), D ** -0.5, 0.125, ((0, 16), (1, 2)))
    w_down = centred(seeds[7], (EXPERTS, D, H), H ** -0.5, 0.21875, ((0, 16), (1, 2)))
    m_in = centred(seeds[8], (EXPERTS, D, 2 * H), 2.0, 12.0, ((0, 16), (1, 2)))
    m_down = centred(seeds[9], (EXPERTS, D, H), 2.0, 12.0, ((0, 16), (1, 2)))
    v_in = jnp.clip(jnp.exp(math.log(400.0) - 4.6051702 * jax.random.uniform(seeds[10], (EXPERTS, D, 2 * H), jnp.float32) ** level_of(seeds[10], (EXPERTS, D, 2 * H), ((0, 16), (1, 2)), -0.2, 0.2)), 4.0, 400.0).astype(jnp.bfloat16)
    v_down = jnp.clip(jnp.exp(math.log(400.0) - 4.6051702 * jax.random.uniform(seeds[11], (EXPERTS, D, H), jnp.float32) ** level_of(seeds[11], (EXPERTS, D, H), ((0, 16), (1, 2)), -0.2, 0.2)), 4.0, 400.0).astype(jnp.bfloat16)
    return dict(tokens=tokens, out_grad=out_grad, expert_ids=expert_ids, gate_probs=gate_probs, held_expert=held_expert, swap_pairs=swap_pairs, w_in=w_in, w_down=w_down, m_in=m_in, m_down=m_down, v_in=v_in, v_down=v_down)


beta_one = 0.9
beta_two = 0.95
learn_rate = 0.01
adam_eps = 1e-08
bias_one = 1.0 - 0.9 ** 10
bias_two = 1.0 - 0.95 ** 10

def expert_pass(rows_x, rows_s, weight_in, weight_down):
    half_width = weight_down.shape[1]
    projected = jnp.dot(rows_x, weight_in, preferred_element_type=jnp.float32)
    gate_part = projected[:, :half_width]
    up_part = projected[:, half_width:]
    sigmoid = jax.nn.sigmoid(gate_part)
    activated = gate_part * sigmoid
    slope_term = sigmoid * (1.0 + gate_part * (1.0 - sigmoid))
    hidden = (activated * up_part).astype(jnp.bfloat16)
    expert_out = lax.dot_general(hidden, weight_down, (((1,), (1,)), ((), ())), preferred_element_type=jnp.float32).astype(jnp.bfloat16)
    hidden_grad = jnp.dot(rows_s, weight_down, preferred_element_type=jnp.float32)
    pre_grad = jnp.concatenate([hidden_grad * up_part * slope_term, hidden_grad * activated], axis=1).astype(jnp.bfloat16)
    row_grad = lax.dot_general(pre_grad, weight_in, (((1,), (1,)), ((), ())), preferred_element_type=jnp.float32).astype(jnp.bfloat16)
    grad_in = lax.dot_general(rows_x, pre_grad, (((0,), (0,)), ((), ())), preferred_element_type=jnp.float32).astype(jnp.bfloat16)
    grad_down = lax.dot_general(rows_s, hidden, (((0,), (0,)), ((), ())), preferred_element_type=jnp.float32).astype(jnp.bfloat16)
    return (row_grad, expert_out, grad_in, grad_down)

def adam_update(weight, first, second, grad):
    first_new = beta_one * first.astype(jnp.float32) + (1.0 - beta_one) * grad
    second_new = beta_two * second.astype(jnp.float32) + (1.0 - beta_two) * grad * grad
    step_size = first_new / bias_one / (jnp.sqrt(second_new / bias_two) + adam_eps)
    weight_new = weight.astype(jnp.float32) - learn_rate * step_size
    return (weight_new.astype(jnp.bfloat16), first_new.astype(jnp.bfloat16), second_new.astype(jnp.bfloat16))

def swap_slots(array, swap_flag):
    partner = jnp.roll(array, EXPERTS // 2, axis=0)
    flag_shape = swap_flag.reshape((-1,) + (1,) * (array.ndim - 1))
    return jnp.where(flag_shape, partner, array)

def reference(tokens, out_grad, expert_ids, gate_probs, held_expert, swap_pairs, w_in, w_down, m_in, m_down, v_in, v_down):
    half_count = EXPERTS // 2
    slot_ids = jnp.arange(EXPERTS, dtype=jnp.int32)
    swap_flag = jnp.any((slot_ids % half_count)[:, None] == swap_pairs[None, :], axis=1)
    held_after = swap_slots(held_expert, swap_flag)
    state_in = swap_slots(w_in, swap_flag)
    state_down = swap_slots(w_down, swap_flag)
    first_in = swap_slots(m_in, swap_flag)
    first_down = swap_slots(m_down, swap_flag)
    second_in = swap_slots(v_in, swap_flag)
    second_down = swap_slots(v_down, swap_flag)
    group_tokens = EXPERTS * TOK_DEV
    picks = group_tokens * TOP
    room = EXPERTS * CAP
    scaled = (gate_probs[:, :, None] * out_grad[:, None, :].astype(jnp.float32)).astype(jnp.bfloat16)
    tokens_grouped = tokens.reshape(N_DP, group_tokens, D)
    scaled_grouped = scaled.reshape(N_DP, picks, D)
    ids_grouped = expert_ids.reshape(N_DP, picks)

    def one_group(expert, weight_in, weight_down, group_x, group_s, group_ids):
        hits = group_ids == expert
        found = jnp.nonzero(hits, size=room, fill_value=0)[0].astype(jnp.int32)
        valid = jnp.arange(room, dtype=jnp.int32) < jnp.sum(hits.astype(jnp.int32))
        rows_x = jnp.where(valid[:, None], group_x[found // TOP], jnp.zeros((), jnp.bfloat16))
        rows_s = jnp.where(valid[:, None], group_s[found], jnp.zeros((), jnp.bfloat16))
        row_grad, expert_out, grad_in, grad_down = expert_pass(rows_x, rows_s, weight_in, weight_down)
        target = jnp.where(valid, found, picks).astype(jnp.int32)
        return (row_grad, expert_out, target, grad_in, grad_down)

    def one_slot(packed):
        expert, weight_in, weight_down = packed

        def per_group(group):
            return one_group(expert, weight_in, weight_down, group[0], group[1], group[2])
        row_grad, expert_out, target, grad_in, grad_down = lax.map(per_group, (tokens_grouped, scaled_grouped, ids_grouped))
        return (row_grad, expert_out, target, lax.optimization_barrier(jnp.sum(grad_in.astype(jnp.float32), axis=0)), lax.optimization_barrier(jnp.sum(grad_down.astype(jnp.float32), axis=0)))
    row_grad, expert_out, target, grad_in, grad_down = lax.map(one_slot, (held_after, state_in, state_down))

    def place(values, where_to):
        flat_pos = where_to.reshape(-1)
        flat_values = values.reshape((flat_pos.shape[0],) + values.shape[2:])
        base = jnp.zeros((picks,) + values.shape[2:], values.dtype)
        return base.at[flat_pos].set(flat_values, mode='drop')
    grads_picked = jax.vmap(place, in_axes=(1, 1))(row_grad, target)
    outs_picked = jax.vmap(place, in_axes=(1, 1))(expert_out, target)
    token_grad = lax.optimization_barrier(jnp.sum(grads_picked.reshape(N_DP, group_tokens, TOP, D).astype(jnp.float32), axis=2)).astype(jnp.bfloat16).reshape(TOKENS, D)
    prob_grad = lax.optimization_barrier(jnp.sum(outs_picked.reshape(TOKENS, TOP, D).astype(jnp.float32) * out_grad[:, None, :].astype(jnp.float32), axis=2))
    new_w_in, new_m_in, new_v_in = adam_update(state_in, first_in, second_in, grad_in)
    new_w_down, new_m_down, new_v_down = adam_update(state_down, first_down, second_down, grad_down)
    return (token_grad, prob_grad, new_w_in, new_w_down, new_m_in, new_m_down, new_v_in, new_v_down)
```

```python
import functools
import itertools
import math

import jax
import jax.numpy as jnp
from jax import lax
from jax.experimental import pallas as pl
from jax.experimental.pallas import tpu as pltpu
from jax.sharding import PartitionSpec as P


beta_one = 0.9
beta_two = 0.95
learn_rate = 0.01
adam_eps = 1e-08
bias_one = 1.0 - 0.9**10
bias_two = 1.0 - 0.95**10
most_branches = 128


def after(value, *others):
    return lax.optimization_barrier((value,) + others)[0]


def inner_slots(experts):
    return 1 << ((experts.bit_length() - 1) // 2)


def swap_subsets(half_axis, pair_count):
    if math.comb(half_axis, pair_count) > most_branches:
        return None
    return list(itertools.combinations(range(half_axis), pair_count))


def subset_index(swap_pairs, subsets):
    if subsets is None:
        return jnp.zeros((), jnp.int32)
    mask = jnp.sum(jnp.left_shift(1, swap_pairs.astype(jnp.int32)))
    masks = jnp.array([sum(1 << p for p in subset) for subset in subsets], jnp.int32)
    numbers = jnp.arange(len(subsets), dtype=jnp.int32)
    return jnp.sum(jnp.where(masks == mask, numbers, 0))


def swapped(x, index, subsets, mine_flag):
    experts = lax.axis_size("expert")
    half_axis = experts // 2
    if subsets is None:
        pairs = [(i, (i + half_axis) % experts) for i in range(experts)]
        return jnp.where(mine_flag, lax.ppermute(x, "expert", pairs), x)

    def branch(subset):
        pairs = [
            (i, (i + half_axis) % experts if i % half_axis in subset else i)
            for i in range(experts)
        ]
        return lambda y: lax.ppermute(y, "expert", pairs)

    return lax.switch(index, [branch(subset) for subset in subsets], x)


def adam_kernel(w_ref, m_ref, v_ref, *refs):
    grads, outs = refs[: len(refs) - 6], refs[len(refs) - 6 :]
    per_weight = len(grads) // 2
    start = 0
    for i in range(2):
        parts = grads[i * per_weight : (i + 1) * per_weight]
        columns = slice(start, start + parts[0].shape[1])
        start = columns.stop
        weight, first, second = (
            r[:, columns].astype(jnp.float32) for r in (w_ref, m_ref, v_ref)
        )
        grad = sum(r[...].astype(jnp.float32) for r in parts)
        first_new = beta_one * first + (1.0 - beta_one) * grad
        second_new = beta_two * second + (1.0 - beta_two) * grad * grad
        scaled = second_new * (1.0 / bias_two)
        denominator = scaled * lax.rsqrt(scaled) + adam_eps
        weight_new = weight - first_new * (learn_rate / bias_one) / denominator
        for out, value in zip(outs[3 * i :], (weight_new, first_new, second_new)):
            out[0] = value.astype(out.dtype)


def adam_update(weight, first, second, grads_in, grads_down):
    rows, columns = weight.shape
    block = math.gcd(rows, 256)
    grads = grads_in + grads_down
    widths = [grads_in[0].shape[1]] * 3 + [grads_down[0].shape[1]] * 3
    return pl.pallas_call(
        adam_kernel,
        grid=(rows // block,),
        in_specs=[pl.BlockSpec((block, columns), lambda i: (i, 0))] * 3
        + [pl.BlockSpec((block, g.shape[1]), lambda i: (i, 0)) for g in grads],
        out_specs=[pl.BlockSpec((1, block, n), lambda i: (0, i, 0)) for n in widths],
        out_shape=[jax.ShapeDtypeStruct((1, rows, n), jnp.bfloat16) for n in widths],
        name="adam",
    )(weight, first, second, *grads)


def lay_kernel(swap_halves, group_ref, x_ref, g_ref, extra_ref, out_ref):
    width = x_ref.shape[1]
    half = width // 2

    def lay(first):
        for base, ref in ((0, x_ref), (width, g_ref)):
            out_ref[:, base : base + half] = ref[:, first : first + half]
            out_ref[:, base + half : base + width] = ref[:, half - first : width - first]

    if swap_halves:
        pl.when(group_ref[0] == 0)(functools.partial(lay, 0))
        pl.when(group_ref[0] != 0)(functools.partial(lay, half))
    else:
        lay(0)
    out_ref[:, 2 * width :] = extra_ref[...]


def lay_rows(swap_halves, group, x, g, extra):
    columns = 2 * x.shape[1] + extra.shape[1]
    vmem = pl.BlockSpec(memory_space=pltpu.VMEM)
    return pl.pallas_call(
        functools.partial(lay_kernel, swap_halves),
        in_specs=[pl.BlockSpec(memory_space=pltpu.SMEM), vmem, vmem, vmem],
        out_specs=vmem,
        out_shape=jax.ShapeDtypeStruct((x.shape[0], columns), x.dtype),
        name="lay_rows",
    )(group.reshape(1), x, g, extra)


def pick_kernel(picker_ref, *refs):
    tables, out_ref = refs[:-1], refs[-1]
    rows = tables[0].shape[0]
    out_ref[...] = sum(
        dot(picker_ref[:, i * rows : (i + 1) * rows], t[...]) for i, t in enumerate(tables)
    ).astype(out_ref.dtype)


def pick_rows(picker, tables):
    rows, columns = tables[0].shape
    lanes = columns // 128
    steps = next(n for n in (3, 4, 2, 5, 1) if lanes % n == 0)
    block = columns // steps
    return pl.pallas_call(
        pick_kernel,
        grid=(steps,),
        in_specs=[pl.BlockSpec(picker.shape, lambda i: (0, 0))]
        + [pl.BlockSpec((rows, block), lambda i: (0, i)) for _ in tables],
        out_specs=pl.BlockSpec((picker.shape[0], block), lambda i: (0, i)),
        out_shape=jax.ShapeDtypeStruct((picker.shape[0], columns), jnp.bfloat16),
        name="pick_rows",
    )(picker, *tables)


def layer_kernel(top_count, outer, expert_ref, rows_hbm, *refs):
    count = (len(refs) - 7) // 2
    weights_hbm, refs = refs[:count], refs[count:]
    back_ref, pre_hbm, hidden_hbm, rows_ref = refs[:4]
    weights, (pre_ref, hidden_ref, sems) = refs[4 : 4 + count], refs[4 + count :]
    piece, half = weights[0].shape[0], weights[0].shape[1] // 3
    width = piece * count
    capacity = back_ref.shape[1]
    inner = back_ref.shape[0] // outer
    copies = []

    def fetch(source, target, columns):
        copies.append(
            pltpu.make_async_copy(
                source.at[:, columns], target.at[:, columns], sems.at[len(copies)]
            )
        )
        copies[-1].start()
        return copies[-1]

    def fetch_weights(base):
        columns = slice(base * half, (base + 1) * half)
        return [fetch(s, t, columns) for s, t in zip(weights_hbm, weights)]

    here_g = fetch(rows_hbm, rows_ref, slice(width, rows_ref.shape[1]))
    here_down = fetch_weights(2)
    here_x = fetch(rows_hbm, rows_ref, slice(0, width))
    here_gate = fetch_weights(0)
    here_up = fetch_weights(1)

    def product(first, base):
        return sum(
            dot(
                rows_ref[:, first + i * piece : first + (i + 1) * piece],
                weights[i][:, base * half : (base + 1) * half],
            )
            for i in range(count)
        )

    for copy in [here_g] + here_down:
        copy.wait()
    extra = rows_ref[:, 2 * width :].astype(jnp.float32)
    row_prob = 0.0
    for k in range(top_count):
        prob = sum(
            extra[:, top_count * (1 + i) + k : top_count * (1 + i) + k + 1] for i in range(3)
        )
        named = extra[:, k : k + 1] == expert_ref[0].astype(jnp.float32)
        row_prob = row_prob + jnp.where(named, prob, 0.0)
    plain_grad = product(width, 2)
    for copy in [here_x] + here_gate:
        copy.wait()
    gate_part = product(0, 0)
    for copy in here_up:
        copy.wait()
    up_part = product(0, 1)
    sigmoid = jax.nn.sigmoid(gate_part)
    activated = gate_part * sigmoid
    slope_term = sigmoid * (1.0 + gate_part * (1.0 - sigmoid))
    hidden = activated * up_part
    prob_grad = jnp.sum(hidden * plain_grad, axis=1, keepdims=True)
    hidden_grad = row_prob * plain_grad
    pre_ref[:, :half] = (hidden_grad * up_part * slope_term).astype(jnp.bfloat16)
    pre_ref[:, half:] = (hidden_grad * activated).astype(jnp.bfloat16)
    hidden_ref[...] = (row_prob * hidden).astype(jnp.bfloat16)
    out_pre = pltpu.make_async_copy(pre_ref, pre_hbm, sems.at[len(copies)])
    out_hidden = pltpu.make_async_copy(hidden_ref, hidden_hbm, sems.at[len(copies) + 1])
    out_pre.start()
    out_hidden.start()

    rest = prob_grad
    lane = lax.broadcasted_iota(jnp.int32, (rest.shape[0], back_ref.shape[2] - width), 1)
    sent = jnp.zeros(lane.shape, jnp.float32)
    for i in range(3):
        part = rest.astype(jnp.bfloat16).astype(jnp.float32)
        sent = jnp.where(lane == i, part, sent)
        rest = rest - part
    sent = sent.astype(jnp.bfloat16)
    places = [
        (o * inner + i, slice((i * outer + o) * capacity, (i * outer + o + 1) * capacity))
        for i in range(inner)
        for o in range(outer)
    ]
    for p in range(count):
        grad = dot_of(pre_ref[...], weights[p][:, : 2 * half], 1).astype(jnp.bfloat16)
        for place, here in places:
            back_ref[place, :, p * piece : (p + 1) * piece] = grad[here, :]
    for place, here in places:
        back_ref[place, :, width:] = sent[here, :]
    out_pre.wait()
    out_hidden.wait()


def layer_rows(rows, parts, my_expert, top_count, half_width, experts, outer):
    room, columns = rows.shape
    width = parts[0].shape[0] * len(parts)
    hbm = pl.BlockSpec(memory_space=pl.ANY)
    shapes = [
        (experts, room // experts, columns - width),
        (room, 2 * half_width),
        (room, half_width),
    ]
    return pl.pallas_call(
        functools.partial(layer_kernel, top_count, outer),
        in_specs=[pl.BlockSpec(memory_space=pltpu.SMEM), hbm] + [hbm] * len(parts),
        out_specs=[pl.BlockSpec(memory_space=pltpu.VMEM), hbm, hbm],
        out_shape=[jax.ShapeDtypeStruct(shape, jnp.bfloat16) for shape in shapes],
        scratch_shapes=[pltpu.VMEM(rows.shape, jnp.bfloat16)]
        + [pltpu.VMEM(w.shape, jnp.bfloat16) for w in parts]
        + [pltpu.VMEM(shape, jnp.bfloat16) for shape in shapes[1:]]
        + [pltpu.SemaphoreType.DMA((4 + 3 * len(parts),))],
        name="layer_rows",
    )(my_expert.reshape(1), rows, *parts)


def dot(a, b):
    return jnp.dot(a, b, preferred_element_type=jnp.float32)


def dot_of(a, b, axis):
    return lax.dot_general(
        a, b, (((axis,), (axis,)), ((), ())), preferred_element_type=jnp.float32
    )


def as_parts(x):
    parts = []
    for _ in range(3):
        parts.append(lax.reduce_precision(x, 8, 7))
        x = x - parts[-1]
    return [part.astype(jnp.bfloat16) for part in parts]


def padded(columns, lanes=128):
    x = jnp.concatenate(columns, axis=1)
    return jnp.pad(x, ((0, 0), (0, -x.shape[1] % lanes)))


def row_places(hit, capacity):
    order = jnp.cumsum(hit.astype(jnp.int32), axis=-1) - 1
    places = jnp.arange(capacity, dtype=jnp.int32)[:, None]
    return hit[..., None, :] & (order[..., None, :] == places)


def body(
    tokens,
    out_grad,
    expert_ids,
    gate_probs,
    held_expert,
    swap_pairs,
    w_in,
    w_down,
    m_in,
    m_down,
    v_in,
    v_down,
):
    experts = lax.axis_size("expert")
    groups = lax.axis_size("dp")
    half_axis = experts // 2
    tok_rows, width = tokens.shape
    top_count = expert_ids.shape[1]
    half_width = w_down.shape[2]
    capacity = max(2, 2 * tok_rows * top_count // experts)
    room = experts * capacity
    inner = inner_slots(experts)
    outer = experts // inner
    me = lax.axis_index("expert")
    my_outer = me // inner
    slot_ids = jnp.arange(experts, dtype=jnp.int32)
    swap_flag = jnp.any((slot_ids % half_axis)[:, None] == swap_pairs[None, :], axis=1)
    mine_flag = swap_flag[me]
    held_after = jnp.where(swap_flag, jnp.roll(held_expert, half_axis), held_expert)
    subsets = swap_subsets(half_axis, swap_pairs.shape[0])
    index = subset_index(swap_pairs, subsets)

    paired = groups == 2
    my_group = lax.axis_index("dp")

    def own_first(x):
        if not paired:
            return [x]
        low, high = x[:, : width // 2], x[:, width // 2 :]
        return [
            jnp.where(my_group == 0, low, high),
            jnp.where(my_group == 0, high, low),
        ]

    extra = padded([expert_ids.astype(jnp.bfloat16)] + as_parts(gate_probs))
    both = lay_rows(paired, my_group, tokens, out_grad, extra)

    def ids_of(x):
        return x[:, 2 * width : 2 * width + top_count].astype(jnp.float32)

    def along(x, bit):
        pairs = [(i, ((i // inner) ^ bit) * inner + i % inner) for i in range(experts)]
        return lax.ppermute(x, "expert", pairs)

    bits = [1 << b for b in reversed(range(outer.bit_length() - 1))]
    tables = {0: both}
    for bit in bits:
        tables[bit] = along(both, bit)
    state_w = jnp.concatenate([w_in[0], w_down[0]], axis=1)
    state_m = jnp.concatenate([m_in[0], m_down[0]], axis=1)
    state_v = jnp.concatenate([v_in[0], v_down[0]], axis=1)
    for offset in sorted(range(1, outer), key=lambda o: (bin(o).count("1"), o)):
        if offset not in tables:
            bit = offset & -offset
            tables[offset] = along(tables[offset ^ bit], bit)
    offsets = list(range(outer))
    tables = [tables[o] for o in offsets]
    index = after(index, *[tables[bit] for bit in bits])

    now_w = swapped(state_w, index, subsets, mine_flag)

    near_experts = lax.dynamic_slice(held_after, (my_outer * inner,), (inner,))
    near_experts = near_experts.astype(jnp.float32)[:, None, None]
    near_ids = jnp.concatenate([ids_of(t) for t in tables], axis=0)
    near_hit = jnp.any(near_ids[None] == near_experts, axis=2)
    near_chosen = row_places(near_hit.reshape(inner, outer, tok_rows), capacity)
    is_block = (jnp.arange(outer)[:, None] ^ my_outer) == jnp.array(offsets)[None, :]
    picker = (
        near_chosen.swapaxes(1, 2)[:, None] & is_block[None, :, None, :, None]
    ).astype(jnp.bfloat16)
    picker = picker.reshape(room, outer * tok_rows)
    send = pick_rows(picker, tables)
    near = [[o * inner + i for i in range(inner)] for o in range(outer)]
    rows = lax.all_to_all(
        send.reshape(inner, outer * capacity, -1),
        "expert",
        split_axis=0,
        concat_axis=0,
        tiled=True,
        axis_index_groups=near,
    ).reshape(room, -1)

    if paired:
        parts = [now_w, lax.ppermute(now_w, "dp", [(0, 1), (1, 0)])]
    else:
        parts = [lax.all_gather(now_w, "dp", axis=0, tiled=True)]
    index = after(index, now_w, send)
    now_m = swapped(state_m, index, subsets, mine_flag)
    rows = after(rows, now_m)

    piece = width // len(parts)
    cut = [rows[:, i * piece : (i + 1) * piece] for i in range(2 * len(parts))]
    rows_x, rows_g = cut[: len(parts)], cut[len(parts) :]
    to_source, pre_grad, scaled_hidden = layer_rows(
        rows, parts, held_after[me], top_count, half_width, experts, outer
    )
    back_grad = lax.all_to_all(
        to_source, "expert", split_axis=0, concat_axis=0, tiled=True
    ).reshape(room, -1)
    if paired:
        far_in = dot_of(rows_x[1], pre_grad, 0).astype(jnp.bfloat16)
        far_down = dot_of(rows_g[1], scaled_hidden, 0).astype(jnp.bfloat16)
        sent_in = lax.ppermute(far_in, "dp", [(0, 1), (1, 0)])
        sent_down = lax.ppermute(far_down, "dp", [(0, 1), (1, 0)])
        near_in = dot_of(rows_x[0], pre_grad, 0).astype(jnp.bfloat16)
        near_down = dot_of(rows_g[0], scaled_hidden, 0).astype(jnp.bfloat16)
        index = after(index, to_source, far_in, far_down, near_in, near_down)
    else:
        grad_in = dot_of(rows_x[0], pre_grad, 0).astype(jnp.bfloat16)
        grad_down = dot_of(rows_g[0], scaled_hidden, 0).astype(jnp.bfloat16)
        sum_in = lax.psum_scatter(grad_in, "dp", scatter_dimension=0, tiled=True)
        sum_down = lax.psum_scatter(grad_down, "dp", scatter_dimension=0, tiled=True)
        grads_in, grads_down = [sum_in], [sum_down]
    now_v = swapped(state_v, index, subsets, mine_flag)
    if paired:
        grads_in, grads_down = [near_in, sent_in], [near_down, sent_down]

    target_slot = jnp.sum(
        jnp.where(held_after[None, None, :] == expert_ids[:, :, None], slot_ids, 0), axis=2
    )
    one_hot = jnp.any(target_slot[:, :, None] == slot_ids, axis=1).astype(jnp.int32)
    earlier = jnp.cumsum(one_hot, axis=0) - one_hot
    position = jnp.sum(
        jnp.where(target_slot[:, :, None] == slot_ids, earlier[:, None, :], 0), axis=2
    )
    back_at = target_slot * capacity + position
    picked = [jnp.take(back_grad, back_at[:, k], axis=0, mode="clip") for k in range(top_count)]
    token_grad = sum(x[:, :width].astype(jnp.float32) for x in picked).astype(jnp.bfloat16)
    token_grad = jnp.concatenate(own_first(token_grad), axis=1)
    prob_grad = jnp.stack(
        [jnp.sum(x[:, width:].astype(jnp.float32), axis=1) for x in picked], axis=1
    )

    new_w_in, new_m_in, new_v_in, new_w_down, new_m_down, new_v_down = adam_update(
        now_w, now_m, now_v, grads_in, grads_down
    )
    return (
        token_grad,
        prob_grad,
        new_w_in,
        new_w_down,
        new_m_in,
        new_m_down,
        new_v_in,
        new_v_down,
    )


def solution(mesh):
    split_rows = P(("dp", "expert"), None)
    split_state = P("expert", "dp", None)
    in_specs = (split_rows,) * 4 + (P(), P()) + (split_state,) * 6
    out_specs = (split_rows,) * 2 + (split_state,) * 6

    return jax.shard_map(body, mesh=mesh, in_specs=in_specs, out_specs=out_specs, check_vma=False)
```

```python
import functools
import itertools
import math

import jax
import jax.numpy as jnp
from jax import lax
from jax.experimental import pallas as pl
from jax.experimental.pallas import tpu as pltpu
from jax.sharding import PartitionSpec as P


beta_one = 0.9
beta_two = 0.95
learn_rate = 0.01
adam_eps = 1e-08
bias_one = 1.0 - 0.9**10
bias_two = 1.0 - 0.95**10
most_branches = 128


def after(value, *others):
    return lax.optimization_barrier((value,) + others)[0]


def inner_slots(experts):
    return 1 << ((experts.bit_length() - 1) // 2)


def swap_subsets(half_axis, pair_count):
    if math.comb(half_axis, pair_count) > most_branches:
        return None
    return list(itertools.combinations(range(half_axis), pair_count))


def subset_index(swap_pairs, subsets):
    if subsets is None:
        return jnp.zeros((), jnp.int32)
    mask = jnp.sum(jnp.left_shift(1, swap_pairs.astype(jnp.int32)))
    masks = jnp.array([sum(1 << p for p in subset) for subset in subsets], jnp.int32)
    numbers = jnp.arange(len(subsets), dtype=jnp.int32)
    return jnp.sum(jnp.where(masks == mask, numbers, 0))


def swapped(x, index, subsets, mine_flag):
    experts = lax.axis_size("expert")
    half_axis = experts // 2
    if subsets is None:
        pairs = [(i, (i + half_axis) % experts) for i in range(experts)]
        return jnp.where(mine_flag, lax.ppermute(x, "expert", pairs), x)

    def branch(subset):
        pairs = [
            (i, (i + half_axis) % experts if i % half_axis in subset else i)
            for i in range(experts)
        ]
        return lambda y: lax.ppermute(y, "expert", pairs)

    return lax.switch(index, [branch(subset) for subset in subsets], x)


def adam_kernel(split, w_ref, m_ref, v_ref, *refs):
    if split:
        early_ref, refs = refs[0], refs[1:]
    grads, outs = refs[: len(refs) - 6], refs[len(refs) - 6 :]
    per_weight = len(grads) // 2
    start = 0
    for i in range(2):
        parts = grads[i * per_weight : (i + 1) * per_weight]
        columns = slice(start, start + parts[0].shape[1])
        start = columns.stop
        weight, first, second = (
            r[:, columns].astype(jnp.float32) for r in (w_ref, m_ref, v_ref)
        )
        if split:
            early = early_ref[:, columns].astype(jnp.float32)
            second = jnp.where(pl.program_id(0) == 0, early, second)
        grad = sum(r[...].astype(jnp.float32) for r in parts)
        first_new = beta_one * first + (1.0 - beta_one) * grad
        second_new = beta_two * second + (1.0 - beta_two) * grad * grad
        scaled = second_new * (1.0 / bias_two)
        denominator = scaled * lax.rsqrt(scaled) + adam_eps
        weight_new = weight - first_new * (learn_rate / bias_one) / denominator
        for out, value in zip(outs[3 * i :], (weight_new, first_new, second_new)):
            out[0] = value.astype(out.dtype)


def adam_update(weight, first, second, early, grads_in, grads_down):
    rows, columns = weight.shape
    block = math.gcd(rows, 256) if early is None else early.shape[0]
    state = pl.BlockSpec((block, columns), lambda i: (i, 0))
    seconds, specs = [second], [state]
    if early is not None:
        seconds = [second, early]
        specs = [
            pl.BlockSpec((block, columns), lambda i: (jnp.maximum(i - 1, 0), 0)),
            pl.BlockSpec((block, columns), lambda i: (0, 0)),
        ]
    grads = grads_in + grads_down
    widths = [grads_in[0].shape[1]] * 3 + [grads_down[0].shape[1]] * 3
    return pl.pallas_call(
        functools.partial(adam_kernel, early is not None),
        grid=(rows // block,),
        in_specs=[state, state]
        + specs
        + [pl.BlockSpec((block, g.shape[1]), lambda i: (i, 0)) for g in grads],
        out_specs=[pl.BlockSpec((1, block, n), lambda i: (0, i, 0)) for n in widths],
        out_shape=[jax.ShapeDtypeStruct((1, rows, n), jnp.bfloat16) for n in widths],
        name="adam",
    )(weight, first, *seconds, *grads)


def lay_kernel(swap_halves, group_ref, x_ref, g_ref, extra_ref, out_ref):
    width = x_ref.shape[1]
    half = width // 2

    def lay(first):
        for base, ref in ((0, x_ref), (width, g_ref)):
            out_ref[:, base : base + half] = ref[:, first : first + half]
            out_ref[:, base + half : base + width] = ref[:, half - first : width - first]

    if swap_halves:
        pl.when(group_ref[0] == 0)(functools.partial(lay, 0))
        pl.when(group_ref[0] != 0)(functools.partial(lay, half))
    else:
        lay(0)
    out_ref[:, 2 * width :] = extra_ref[...]


def lay_rows(swap_halves, group, x, g, extra):
    columns = 2 * x.shape[1] + extra.shape[1]
    vmem = pl.BlockSpec(memory_space=pltpu.VMEM)
    return pl.pallas_call(
        functools.partial(lay_kernel, swap_halves),
        in_specs=[pl.BlockSpec(memory_space=pltpu.SMEM), vmem, vmem, vmem],
        out_specs=vmem,
        out_shape=jax.ShapeDtypeStruct((x.shape[0], columns), x.dtype),
        name="lay_rows",
    )(group.reshape(1), x, g, extra)


def pick_kernel(picker_ref, *refs):
    tables, out_ref = refs[:-1], refs[-1]
    rows = tables[0].shape[0]
    out_ref[...] = sum(
        dot(picker_ref[:, i * rows : (i + 1) * rows], t[...]) for i, t in enumerate(tables)
    ).astype(out_ref.dtype)


def pick_rows(picker, tables):
    rows, columns = tables[0].shape
    lanes = columns // 128
    steps = next(n for n in (3, 4, 2, 5, 1) if lanes % n == 0)
    block = columns // steps
    return pl.pallas_call(
        pick_kernel,
        grid=(steps,),
        in_specs=[pl.BlockSpec(picker.shape, lambda i: (0, 0))]
        + [pl.BlockSpec((rows, block), lambda i: (0, i)) for _ in tables],
        out_specs=pl.BlockSpec((picker.shape[0], block), lambda i: (0, i)),
        out_shape=jax.ShapeDtypeStruct((picker.shape[0], columns), jnp.bfloat16),
        name="pick_rows",
    )(picker, *tables)


def layer_kernel(top_count, outer, expert_ref, rows_hbm, *refs):
    count = (len(refs) - 7) // 2
    weights_hbm, refs = refs[:count], refs[count:]
    back_ref, pre_hbm, hidden_hbm, rows_ref = refs[:4]
    weights, (pre_ref, hidden_ref, sems) = refs[4 : 4 + count], refs[4 + count :]
    piece, half = weights[0].shape[0], weights[0].shape[1] // 3
    width = piece * count
    capacity = back_ref.shape[1]
    inner = back_ref.shape[0] // outer
    copies = []

    def fetch(source, target, columns):
        copies.append(
            pltpu.make_async_copy(
                source.at[:, columns], target.at[:, columns], sems.at[len(copies)]
            )
        )
        copies[-1].start()
        return copies[-1]

    def fetch_weights(base):
        columns = slice(base * half, (base + 1) * half)
        return [fetch(s, t, columns) for s, t in zip(weights_hbm, weights)]

    here_g = fetch(rows_hbm, rows_ref, slice(width, rows_ref.shape[1]))
    here_down = fetch_weights(2)
    here_x = fetch(rows_hbm, rows_ref, slice(0, width))
    here_gate = fetch_weights(0)
    here_up = fetch_weights(1)

    def product(first, base):
        return sum(
            dot(
                rows_ref[:, first + i * piece : first + (i + 1) * piece],
                weights[i][:, base * half : (base + 1) * half],
            )
            for i in range(count)
        )

    for copy in [here_g] + here_down:
        copy.wait()
    extra = rows_ref[:, 2 * width :].astype(jnp.float32)
    row_prob = 0.0
    for k in range(top_count):
        prob = sum(
            extra[:, top_count * (1 + i) + k : top_count * (1 + i) + k + 1] for i in range(3)
        )
        named = extra[:, k : k + 1] == expert_ref[0].astype(jnp.float32)
        row_prob = row_prob + jnp.where(named, prob, 0.0)
    plain_grad = product(width, 2)
    for copy in [here_x] + here_gate:
        copy.wait()
    gate_part = product(0, 0)
    for copy in here_up:
        copy.wait()
    up_part = product(0, 1)
    sigmoid = jax.nn.sigmoid(gate_part)
    activated = gate_part * sigmoid
    slope_term = sigmoid * (1.0 + gate_part * (1.0 - sigmoid))
    hidden = activated * up_part
    prob_grad = jnp.sum(hidden * plain_grad, axis=1, keepdims=True)
    hidden_grad = row_prob * plain_grad
    pre_ref[:, :half] = (hidden_grad * up_part * slope_term).astype(jnp.bfloat16)
    pre_ref[:, half:] = (hidden_grad * activated).astype(jnp.bfloat16)
    hidden_ref[...] = (row_prob * hidden).astype(jnp.bfloat16)
    out_pre = pltpu.make_async_copy(pre_ref, pre_hbm, sems.at[len(copies)])
    out_hidden = pltpu.make_async_copy(hidden_ref, hidden_hbm, sems.at[len(copies) + 1])
    out_pre.start()
    out_hidden.start()

    rest = prob_grad
    lane = lax.broadcasted_iota(jnp.int32, (rest.shape[0], back_ref.shape[2] - width), 1)
    sent = jnp.zeros(lane.shape, jnp.float32)
    for i in range(3):
        part = rest.astype(jnp.bfloat16).astype(jnp.float32)
        sent = jnp.where(lane == i, part, sent)
        rest = rest - part
    sent = sent.astype(jnp.bfloat16)
    places = [
        (o * inner + i, slice((i * outer + o) * capacity, (i * outer + o + 1) * capacity))
        for i in range(inner)
        for o in range(outer)
    ]
    for p in range(count):
        grad = dot_of(pre_ref[...], weights[p][:, : 2 * half], 1).astype(jnp.bfloat16)
        for place, here in places:
            back_ref[place, :, p * piece : (p + 1) * piece] = grad[here, :]
    for place, here in places:
        back_ref[place, :, width:] = sent[here, :]
    out_pre.wait()
    out_hidden.wait()


def layer_rows(rows, parts, my_expert, top_count, half_width, experts, outer):
    room, columns = rows.shape
    width = parts[0].shape[0] * len(parts)
    hbm = pl.BlockSpec(memory_space=pl.ANY)
    shapes = [
        (experts, room // experts, columns - width),
        (room, 2 * half_width),
        (room, half_width),
    ]
    return pl.pallas_call(
        functools.partial(layer_kernel, top_count, outer),
        in_specs=[pl.BlockSpec(memory_space=pltpu.SMEM), hbm] + [hbm] * len(parts),
        out_specs=[pl.BlockSpec(memory_space=pltpu.VMEM), hbm, hbm],
        out_shape=[jax.ShapeDtypeStruct(shape, jnp.bfloat16) for shape in shapes],
        scratch_shapes=[pltpu.VMEM(rows.shape, jnp.bfloat16)]
        + [pltpu.VMEM(w.shape, jnp.bfloat16) for w in parts]
        + [pltpu.VMEM(shape, jnp.bfloat16) for shape in shapes[1:]]
        + [pltpu.SemaphoreType.DMA((4 + 3 * len(parts),))],
        name="layer_rows",
    )(my_expert.reshape(1), rows, *parts)


def dot(a, b):
    return jnp.dot(a, b, preferred_element_type=jnp.float32)


def dot_of(a, b, axis):
    return lax.dot_general(
        a, b, (((axis,), (axis,)), ((), ())), preferred_element_type=jnp.float32
    )


def as_parts(x):
    parts = []
    for _ in range(3):
        parts.append(lax.reduce_precision(x, 8, 7))
        x = x - parts[-1]
    return [part.astype(jnp.bfloat16) for part in parts]


def padded(columns, lanes=128):
    x = jnp.concatenate(columns, axis=1)
    return jnp.pad(x, ((0, 0), (0, -x.shape[1] % lanes)))


def row_places(hit, capacity):
    order = jnp.cumsum(hit.astype(jnp.int32), axis=-1) - 1
    places = jnp.arange(capacity, dtype=jnp.int32)[:, None]
    return hit[..., None, :] & (order[..., None, :] == places)


def body(
    tokens,
    out_grad,
    expert_ids,
    gate_probs,
    held_expert,
    swap_pairs,
    w_in,
    w_down,
    m_in,
    m_down,
    v_in,
    v_down,
):
    experts = lax.axis_size("expert")
    groups = lax.axis_size("dp")
    half_axis = experts // 2
    tok_rows, width = tokens.shape
    top_count = expert_ids.shape[1]
    half_width = w_down.shape[2]
    capacity = max(2, 2 * tok_rows * top_count // experts)
    room = experts * capacity
    inner = inner_slots(experts)
    outer = experts // inner
    me = lax.axis_index("expert")
    my_outer = me // inner
    slot_ids = jnp.arange(experts, dtype=jnp.int32)
    swap_flag = jnp.any((slot_ids % half_axis)[:, None] == swap_pairs[None, :], axis=1)
    mine_flag = swap_flag[me]
    held_after = jnp.where(swap_flag, jnp.roll(held_expert, half_axis), held_expert)
    subsets = swap_subsets(half_axis, swap_pairs.shape[0])
    index = subset_index(swap_pairs, subsets)

    paired = groups == 2
    my_group = lax.axis_index("dp")

    def own_first(x):
        if not paired:
            return [x]
        low, high = x[:, : width // 2], x[:, width // 2 :]
        return [
            jnp.where(my_group == 0, low, high),
            jnp.where(my_group == 0, high, low),
        ]

    extra = padded([expert_ids.astype(jnp.bfloat16)] + as_parts(gate_probs))
    both = lay_rows(paired, my_group, tokens, out_grad, extra)

    def ids_of(x):
        return x[:, 2 * width : 2 * width + top_count].astype(jnp.float32)

    def along(x, bit):
        pairs = [(i, ((i // inner) ^ bit) * inner + i % inner) for i in range(experts)]
        return lax.ppermute(x, "expert", pairs)

    bits = [1 << b for b in reversed(range(outer.bit_length() - 1))]
    tables = {0: both}
    for bit in bits:
        tables[bit] = along(both, bit)
    state_w = jnp.concatenate([w_in[0], w_down[0]], axis=1)
    state_m = jnp.concatenate([m_in[0], m_down[0]], axis=1)
    early_rows = 0 if subsets is None else w_in.shape[1] // 8
    early_v = None
    state_v = jnp.concatenate([v_in[0, early_rows:], v_down[0, early_rows:]], axis=1)
    for offset in sorted(range(1, outer), key=lambda o: (bin(o).count("1"), o)):
        if offset not in tables:
            bit = offset & -offset
            tables[offset] = along(tables[offset ^ bit], bit)
    offsets = list(range(outer))
    tables = [tables[o] for o in offsets]
    index = after(index, *[tables[bit] for bit in bits])

    now_w = swapped(state_w, index, subsets, mine_flag)

    near_experts = lax.dynamic_slice(held_after, (my_outer * inner,), (inner,))
    near_experts = near_experts.astype(jnp.float32)[:, None, None]
    near_ids = jnp.concatenate([ids_of(t) for t in tables], axis=0)
    near_hit = jnp.any(near_ids[None] == near_experts, axis=2)
    near_chosen = row_places(near_hit.reshape(inner, outer, tok_rows), capacity)
    is_block = (jnp.arange(outer)[:, None] ^ my_outer) == jnp.array(offsets)[None, :]
    picker = (
        near_chosen.swapaxes(1, 2)[:, None] & is_block[None, :, None, :, None]
    ).astype(jnp.bfloat16)
    picker = picker.reshape(room, outer * tok_rows)
    send = pick_rows(picker, tables)
    near = [[o * inner + i for i in range(inner)] for o in range(outer)]
    rows = lax.all_to_all(
        send.reshape(inner, outer * capacity, -1),
        "expert",
        split_axis=0,
        concat_axis=0,
        tiled=True,
        axis_index_groups=near,
    ).reshape(room, -1)

    if paired:
        parts = [now_w, lax.ppermute(now_w, "dp", [(0, 1), (1, 0)])]
    else:
        parts = [lax.all_gather(now_w, "dp", axis=0, tiled=True)]
    index = after(index, now_w, send)
    now_m = swapped(state_m, index, subsets, mine_flag)
    rows = after(rows, now_m)
    if early_rows:
        own_v = jnp.concatenate([v_in[0, :early_rows], v_down[0, :early_rows]], axis=1)
        own_v = own_v + 0.0 * now_m[:early_rows]
        early_v = lax.ppermute(
            own_v, "expert", [(i, (i + half_axis) % experts) for i in range(experts)]
        )
        early_v = jnp.where(mine_flag, early_v, own_v)

    piece = width // len(parts)
    cut = [rows[:, i * piece : (i + 1) * piece] for i in range(2 * len(parts))]
    rows_x, rows_g = cut[: len(parts)], cut[len(parts) :]
    to_source, pre_grad, scaled_hidden = layer_rows(
        rows, parts, held_after[me], top_count, half_width, experts, outer
    )
    back_grad = lax.all_to_all(
        to_source, "expert", split_axis=0, concat_axis=0, tiled=True
    ).reshape(room, -1)
    if paired:
        far_in = dot_of(rows_x[1], pre_grad, 0).astype(jnp.bfloat16)
        far_down = dot_of(rows_g[1], scaled_hidden, 0).astype(jnp.bfloat16)
        sent_in = lax.ppermute(far_in, "dp", [(0, 1), (1, 0)])
        sent_down = lax.ppermute(far_down, "dp", [(0, 1), (1, 0)])
        near_in = dot_of(rows_x[0], pre_grad, 0).astype(jnp.bfloat16)
        near_down = dot_of(rows_g[0], scaled_hidden, 0).astype(jnp.bfloat16)
        index = after(index, to_source, far_in, far_down, near_in, near_down)
    else:
        grad_in = dot_of(rows_x[0], pre_grad, 0).astype(jnp.bfloat16)
        grad_down = dot_of(rows_g[0], scaled_hidden, 0).astype(jnp.bfloat16)
        sum_in = lax.psum_scatter(grad_in, "dp", scatter_dimension=0, tiled=True)
        sum_down = lax.psum_scatter(grad_down, "dp", scatter_dimension=0, tiled=True)
        grads_in, grads_down = [sum_in], [sum_down]
    now_v = swapped(state_v, index, subsets, mine_flag)
    if paired:
        grads_in, grads_down = [near_in, sent_in], [near_down, sent_down]

    target_slot = jnp.sum(
        jnp.where(held_after[None, None, :] == expert_ids[:, :, None], slot_ids, 0), axis=2
    )
    one_hot = jnp.any(target_slot[:, :, None] == slot_ids, axis=1).astype(jnp.int32)
    earlier = jnp.cumsum(one_hot, axis=0) - one_hot
    position = jnp.sum(
        jnp.where(target_slot[:, :, None] == slot_ids, earlier[:, None, :], 0), axis=2
    )
    back_at = target_slot * capacity + position
    picked = [jnp.take(back_grad, back_at[:, k], axis=0, mode="clip") for k in range(top_count)]
    token_grad = sum(x[:, :width].astype(jnp.float32) for x in picked).astype(jnp.bfloat16)
    token_grad = jnp.concatenate(own_first(token_grad), axis=1)
    prob_grad = jnp.stack(
        [jnp.sum(x[:, width:].astype(jnp.float32), axis=1) for x in picked], axis=1
    )

    new_w_in, new_m_in, new_v_in, new_w_down, new_m_down, new_v_down = adam_update(
        now_w, now_m, now_v, early_v, grads_in, grads_down
    )
    return (
        token_grad,
        prob_grad,
        new_w_in,
        new_w_down,
        new_m_in,
        new_m_down,
        new_v_in,
        new_v_down,
    )


def solution(mesh):
    split_rows = P(("dp", "expert"), None)
    split_state = P("expert", "dp", None)
    in_specs = (split_rows,) * 4 + (P(), P()) + (split_state,) * 6
    out_specs = (split_rows,) * 2 + (split_state,) * 6

    return jax.shard_map(body, mesh=mesh, in_specs=in_specs, out_specs=out_specs, check_vma=False)
```
